32 devices in a mesh: batch: 1 (over z), row: 4 (over y), col: 8 (over x, core).
Axes of the slice: x: 4, y: 4, z: 1, core: 2. Of those that a mesh axis runs over, the one named last changes fastest.
The devices are a block of a 4x4x8 slice.
Arguments:
- lower_tri: bfloat16 [6144, 6144], P(('batch', 'row'), 'col')
- right_side: bfloat16 [6144, 32768], P(('batch', 'row'), 'col')
- grad_out: bfloat16 [6144, 32768], P(('batch', 'row'), 'col')
Outputs:
- output 1: bfloat16 [6144, 32768], P(('batch', 'row'), 'col')
- output 2: bfloat16 [6144, 6144], P(('batch', 'row'), 'col')
All inputs are finite; a program needn't handle non-finite values.
Results may differ from the reference program's by a relative error of at most 0.001.
Values are sent between devices in bfloat16 or wider.
A program may use at most 768 MiB of HBM per device.

```python
import jax
import jax.numpy as jnp

MAT_ORDER = 6144
BLOCK_SIZE = 256
RHS_COLS = 32768
MESH_ROWS = 4
MESH_COLS = 8
ROW_BLOCKS = MAT_ORDER // (BLOCK_SIZE * MESH_ROWS)
COL_BLOCKS = MAT_ORDER // (BLOCK_SIZE * MESH_COLS)


def rows_to_global(stored):
    num_cols = stored.shape[1]
    return stored.reshape(MESH_ROWS, ROW_BLOCKS, BLOCK_SIZE, num_cols).transpose(1, 0, 2, 3).reshape(MAT_ORDER, num_cols)


def rows_to_stored(natural):
    num_cols = natural.shape[1]
    return natural.reshape(ROW_BLOCKS, MESH_ROWS, BLOCK_SIZE, num_cols).transpose(1, 0, 2, 3).reshape(MAT_ORDER, num_cols)


def cols_to_global(stored):
    num_rows = stored.shape[0]
    return stored.reshape(num_rows, MESH_COLS, COL_BLOCKS, BLOCK_SIZE).transpose(0, 2, 1, 3).reshape(num_rows, MAT_ORDER)


def cols_to_stored(natural):
    num_rows = natural.shape[0]
    return natural.reshape(num_rows, COL_BLOCKS, MESH_COLS, BLOCK_SIZE).transpose(0, 2, 1, 3).reshape(num_rows, MAT_ORDER)


def setup_inputs(seed: int = 0, part: int = 0) -> dict:
    base_key = jax.random.fold_in(jax.random.key(seed), part)
    key_lower, key_right, key_grad = jax.random.split(base_key, 3)
    lower_mat = jax.random.normal(key_lower, (MAT_ORDER, MAT_ORDER), jnp.float32) * (MAT_ORDER ** -0.5)
    lower_mat = jnp.tril(lower_mat).astype(jnp.bfloat16)
    right_mat = jax.random.normal(key_right, (MAT_ORDER, RHS_COLS), jnp.float32) * (RHS_COLS ** -0.5)
    grad_mat = jax.random.normal(key_grad, (MAT_ORDER, RHS_COLS), jnp.float32)
    return {
        "lower_tri": cols_to_stored(rows_to_stored(lower_mat)),
        "right_side": rows_to_stored(right_mat.astype(jnp.bfloat16)),
        "grad_out": rows_to_stored(grad_mat.astype(jnp.bfloat16)),
    }


def reference(lower_tri, right_side, grad_out):
    lower_mat = cols_to_global(rows_to_global(lower_tri))
    right_mat = rows_to_global(right_side)
    grad_mat = rows_to_global(grad_out)
    grad_right = jnp.dot(lower_mat.T, grad_mat, preferred_element_type=jnp.float32)
    grad_lower = jnp.tril(jnp.dot(grad_mat, right_mat.T, preferred_element_type=jnp.float32))
    return (rows_to_stored(grad_right.astype(jnp.bfloat16)), cols_to_stored(rows_to_stored(grad_lower.astype(jnp.bfloat16))))
```

```python
import jax
import jax.numpy as jnp
from jax import lax
from jax.sharding import PartitionSpec as P


BLOCK_SIZE = 256


def solution(mesh):
    mesh_rows = mesh.shape["row"]
    mesh_cols = mesh.shape["col"]
    halves = mesh_cols // mesh_rows
    block_spec = P(("batch", "row"), "col")
    up = [(row, (row + 1) % mesh_rows) for row in range(mesh_rows)]
    down = [(row, (row - 1) % mesh_rows) for row in range(mesh_rows)]

    spread = []
    collect = [[] for _ in range(halves)]
    for row in range(mesh_rows):
        for col in range(mesh_cols):
            home, half = col % mesh_rows, col // mesh_rows
            spread.append((row * mesh_cols + col, home * mesh_cols + half * mesh_rows + (row - home) % mesh_rows))
            rel, part = col // halves, col % halves
            for turn in range(halves):
                owner = (row + rel) % mesh_rows * mesh_cols + row + mesh_rows * ((part + turn) % halves)
                collect[turn].append((row * mesh_cols + col, owner))

    def shards(lower_tri, right_side, grad_out):
        rows_here, cols_here = lower_tri.shape
        num_groups = rows_here // BLOCK_SIZE
        num_supers = num_groups // halves
        my_col = lax.axis_index("col")
        my_half = my_col // mesh_rows
        my_part = my_col % halves

        own = [grad_out[group * BLOCK_SIZE:(group + 1) * BLOCK_SIZE] for group in range(num_groups)]
        near = {}
        far = {}
        panels = {
            sup: lower_tri[sup * halves * BLOCK_SIZE:(sup + 1) * halves * BLOCK_SIZE, :(sup + 1) * BLOCK_SIZE]
            for sup in range(num_supers)
        }
        totals = {}
        sends = {}
        received = {}
        state = {"out": jnp.zeros(right_side.shape, jnp.bfloat16)}

        def send_own(group):
            near[group] = (lax.ppermute(own[group], "row", up), lax.ppermute(own[group], "row", down))

        def spread_panel(sup):
            panel = lax.ppermute(panels[sup], ("row", "col"), spread)
            panels[sup] = lax.all_gather(panel, "col", axis=0)

        def forward(group):
            waits = list(near[group])
            later = group - 2
            if later >= 0:
                waits.append(own[later])
            if group + 2 in totals:
                waits.append(totals[group + 2])
            waits = list(lax.optimization_barrier(tuple(waits)))
            prev_block, next_block = near[group] = (waits.pop(0), waits.pop(0))
            far[group] = (
                lax.ppermute(prev_block[:BLOCK_SIZE // 2], "row", up),
                lax.ppermute(next_block[BLOCK_SIZE // 2:], "row", down),
            )
            if later >= 0:
                own[later] = waits.pop(0)
                send_own(later)
            if group + 2 in totals:
                totals[group + 2] = waits.pop(0)

        def collect_lower(group):
            received[group] = [lax.ppermute(send, ("row", "col"), collect[turn]) for turn, send in enumerate(sends[group])]

        def compute(group):
            width = (group + 1) * BLOCK_SIZE
            sup = group // halves
            waits = [own[group], near[group][1], *far[group], near[group][0], panels[sup]]
            if group > 0:
                waits += near[group - 1]
            if group + 1 in totals:
                waits.append(totals[group + 1])
            if group + 2 in sends:
                waits += sends[group + 2]
            waits = list(lax.optimization_barrier(tuple(waits)))
            blocks, panels[sup] = waits[:5], waits[5]
            waits = waits[6:]
            if group > 0:
                near[group - 1] = (waits.pop(0), waits.pop(0))
            if group + 1 in totals:
                totals[group + 1] = waits.pop(0)
            if group + 2 in sends:
                sends[group + 2] = waits
                collect_lower(group + 2)

            panel = panels[sup].reshape(halves, mesh_rows, halves, BLOCK_SIZE, sup + 1, BLOCK_SIZE)[:, :, group % halves]
            panel = panel.transpose(1, 2, 3, 0, 4).reshape(mesh_rows * BLOCK_SIZE, (sup + 1) * halves * BLOCK_SIZE)
            grad_rows = jnp.concatenate(blocks, axis=0)
            lower_part = lax.dot_general(
                grad_rows, right_side[:width], (((1,), (1,)), ((), ())), preferred_element_type=jnp.float32
            )
            grad_rows, lower_part = lax.optimization_barrier((grad_rows, lower_part))
            lower_mine = lax.psum_scatter(lower_part, "col", scatter_dimension=0, tiled=True)
            lower_mine = lower_mine.astype(jnp.bfloat16)
            total = lax.dot_general(
                panel[:, :width], grad_rows, (((0,), (0,)), ((), ())), preferred_element_type=jnp.float32
            )
            if group + 1 in totals:
                total = totals[group + 1][:width] + total
            totals[group] = total
            done = total[group * BLOCK_SIZE:].astype(jnp.bfloat16)
            state["out"] = lax.dynamic_update_slice(state["out"], done, (group * BLOCK_SIZE, 0))

            lower_mine = jnp.pad(lower_mine, ((0, 0), (0, (sup + 1) * halves * BLOCK_SIZE - width)))
            lower_mine = lower_mine.reshape(-1, sup + 1, halves, BLOCK_SIZE)
            pieces = [lower_mine[:, :, half].reshape(-1, (sup + 1) * BLOCK_SIZE) for half in range(halves)]
            sends[group] = []
            for turn in range(halves):
                send = pieces[turn]
                for part in range(1, halves):
                    send = jnp.where(my_part == part, pieces[(part + turn) % halves], send)
                sends[group].append(send)

        for sup in reversed(range(num_supers)):
            spread_panel(sup)
        send_own(num_groups - 1)
        send_own(num_groups - 2)
        forward(num_groups - 1)
        for group in reversed(range(num_groups)):
            if group > 0:
                forward(group - 1)
            compute(group)
        collect_lower(1)
        collect_lower(0)

        lower_rows = []
        for group in range(num_groups):
            for part in range(halves):
                piece = received[group][0]
                for turn in range(1, halves):
                    piece = jnp.where((my_half - part) % halves == turn, received[group][turn], piece)
                lower_rows.append(jnp.pad(piece, ((0, 0), (0, cols_here - piece.shape[1]))))
        grad_lower = jnp.concatenate(lower_rows, axis=0)
        row_pos = jnp.arange(rows_here)[:, None]
        col_pos = jnp.arange(cols_here)[None, :]
        row_global = (row_pos // BLOCK_SIZE * mesh_rows + lax.axis_index("row")) * BLOCK_SIZE + row_pos % BLOCK_SIZE
        col_global = (col_pos // BLOCK_SIZE * mesh_cols + my_col) * BLOCK_SIZE + col_pos % BLOCK_SIZE
        grad_lower = jnp.where(row_global >= col_global, grad_lower, 0.0).astype(jnp.bfloat16)
        return state["out"], grad_lower

    return jax.shard_map(shards, mesh=mesh, in_specs=(block_spec, block_spec, block_spec), out_specs=(block_spec, block_spec), check_vma=False)
```

```python
import functools

import jax
import jax.numpy as jnp
from jax import lax
from jax.experimental import pallas as pl
from jax.experimental.pallas import tpu as pltpu
from jax.sharding import PartitionSpec as P


BLOCK_SIZE = 256
PIECE = 512


def group_kernel(group, halves, has_total, *refs):
    refs = list(refs)
    block_refs = [refs.pop(0) for _ in range(4)]
    panel_ref, side_ref = refs.pop(0), refs.pop(0)
    total_ref = refs.pop(0) if has_total else None
    if has_total:
        refs.pop(0)
    lower_ref, right_ref = refs.pop(0), refs.pop(0)
    next_ref = refs.pop(0) if group else None
    turned, rows = refs
    mesh_rows = len(block_refs)
    size = block_refs[0].shape[0]
    turns = lower_ref.shape[1] // (halves * size)

    def place(idx):
        return slice((idx % halves * turns + idx // halves) * size, (idx % halves * turns + idx // halves + 1) * size)

    @pl.when(pl.program_id(0) == 0)
    def _():
        lower_ref[...] = jnp.zeros_like(lower_ref)
        for idx in range(group + 1):
            for rel in range(mesh_rows):
                tile = panel_ref[idx % halves * mesh_rows + rel, :, idx // halves * size:(idx // halves + 1) * size]
                turned[idx * size:(idx + 1) * size, rel * size:(rel + 1) * size] = tile.T

    for rel in range(mesh_rows):
        rows[rel * size:(rel + 1) * size, :] = block_refs[rel][...]
    for idx in range(group + 1):
        here = slice(idx * size, (idx + 1) * size)
        lower_ref[:, place(idx)] += lax.dot_general(
            rows[...], side_ref[here, :], (((1,), (1,)), ((), ())), preferred_element_type=jnp.float32
        )
        share = jnp.dot(turned[here, :], rows[...], preferred_element_type=jnp.float32)
        if has_total:
            share = total_ref[here, :] + share
        if idx == group:
            right_ref[...] = share.astype(right_ref.dtype)
        else:
            next_ref[here, :] = share


def run_group(group, halves, blocks, panel, side, total, right):
    size = blocks[1].shape[0]
    num_cols = side.shape[1]
    width = (group + 1) * size
    wide = -(-(group + 1) // halves) * halves * size
    depth = panel.shape[1] // halves
    piece = min(PIECE, num_cols)
    has_total = total is not None
    in_specs = [pl.BlockSpec((size, piece), lambda j: (group, j))]
    in_specs += [pl.BlockSpec((size, piece), lambda j: (0, j))] * 3
    in_specs += [
        pl.BlockSpec((panel.shape[0], depth, panel.shape[2]), lambda j: (0, group % halves, 0)),
        pl.BlockSpec((width, piece), lambda j: (0, j)),
    ]
    args = [*blocks, panel, side]
    aliases = {}
    if has_total:
        in_specs += [pl.BlockSpec((width, piece), lambda j: (0, j)), pl.BlockSpec(memory_space=pl.ANY)]
        args += [total, right]
        aliases = {len(args) - 1: 1}
    out_shape = [
        jax.ShapeDtypeStruct((4 * size, wide), jnp.float32),
        jax.ShapeDtypeStruct(side.shape, jnp.bfloat16),
    ]
    out_specs = [
        pl.BlockSpec((4 * size, wide), lambda j: (0, 0)),
        pl.BlockSpec((size, piece), lambda j: (group, j)),
    ]
    if group:
        out_shape.append(jax.ShapeDtypeStruct((group * size, num_cols), jnp.float32))
        out_specs.append(pl.BlockSpec((group * size, piece), lambda j: (0, j)))
    return pl.pallas_call(
        functools.partial(group_kernel, group, halves, has_total),
        grid=(num_cols // piece,),
        in_specs=in_specs,
        out_specs=out_specs,
        out_shape=out_shape,
        scratch_shapes=[pltpu.VMEM((width, 4 * size), jnp.bfloat16), pltpu.VMEM((4 * size, piece), jnp.bfloat16)],
        input_output_aliases=aliases,
        compiler_params=pltpu.CompilerParams(vmem_limit_bytes=56 * 1024 * 1024),
        cost_estimate=pl.CostEstimate(
            flops=4 * 4 * size * width * num_cols, bytes_accessed=num_cols * (12 * size + 10 * width), transcendentals=0
        ),
    )(*args)


def solution(mesh):
    mesh_rows = mesh.shape["row"]
    mesh_cols = mesh.shape["col"]
    halves = mesh_cols // mesh_rows
    block_spec = P(("batch", "row"), "col")
    up = [(row, (row + 1) % mesh_rows) for row in range(mesh_rows)]
    down = [(row, (row - 1) % mesh_rows) for row in range(mesh_rows)]

    spread = []
    collect = [[] for _ in range(halves)]
    for row in range(mesh_rows):
        for col in range(mesh_cols):
            home, half = col % mesh_rows, col // mesh_rows
            spread.append((row * mesh_cols + col, home * mesh_cols + half * mesh_rows + (row - home) % mesh_rows))
            rel, part = col // halves, col % halves
            for turn in range(halves):
                owner = (row + rel) % mesh_rows * mesh_cols + row + mesh_rows * ((part + turn) % halves)
                collect[turn].append((row * mesh_cols + col, owner))

    def shards(lower_tri, right_side, grad_out):
        rows_here, cols_here = lower_tri.shape
        num_groups = rows_here // BLOCK_SIZE
        num_supers = num_groups // halves
        my_col = lax.axis_index("col")
        my_half = my_col // mesh_rows
        my_part = my_col % halves

        own = [grad_out[group * BLOCK_SIZE:(group + 1) * BLOCK_SIZE] for group in range(num_groups)]
        near = {}
        far = {}
        panels = {
            sup: lower_tri[sup * halves * BLOCK_SIZE:(sup + 1) * halves * BLOCK_SIZE, :(sup + 1) * BLOCK_SIZE]
            for sup in range(num_supers)
        }
        totals = {}
        lowers = {}
        sums = {}
        state = {"right": None}

        def send_own(group):
            near[group] = (lax.ppermute(own[group], "row", up), lax.ppermute(own[group], "row", down))

        def spread_panel(sup):
            panel = lax.ppermute(panels[sup], ("row", "col"), spread)
            panels[sup] = lax.all_gather(panel, "col", axis=0)

        def forward(group):
            waits = list(near[group])
            later = group - 2
            if later >= 0:
                waits.append(own[later])
            if group + 2 in totals:
                waits.append(totals[group + 2])
            waits = list(lax.optimization_barrier(tuple(waits)))
            near[group] = (waits.pop(0), waits.pop(0))
            if group % 2:
                far[group] = lax.ppermute(near[group][0], "row", up)
            else:
                far[group] = lax.ppermute(near[group][1], "row", down)
            if later >= 0:
                own[later] = waits.pop(0)
                send_own(later)
            if group + 2 in totals:
                totals[group + 2] = waits.pop(0)

        def choose(values, turn):
            width = values.shape[1] // halves
            chosen = values[:, turn * width:(turn + 1) * width]
            for part in range(1, halves):
                start = (part + turn) % halves * width
                chosen = jnp.where(my_part == part, values[:, start:start + width], chosen)
            return chosen.astype(jnp.bfloat16)

        def collect_lower(sends):
            return [lax.ppermute(send, ("row", "col"), collect[turn]) for turn, send in enumerate(sends)]

        def by_part(turns):
            ordered = []
            for part in range(halves):
                piece = turns[0]
                for turn in range(1, halves):
                    piece = jnp.where((my_half - part) % halves == turn, turns[turn], piece)
                ordered.append(piece)
            return ordered

        def widen(value):
            return jnp.pad(value, ((0, 0), (0, cols_here - value.shape[1])))

        def compute(group):
            sup = group // halves
            waits = [near[group][1], far[group], near[group][0], panels[sup]]
            if group > 0:
                waits += near[group - 1]
            if group + 1 in totals:
                waits.append(totals[group + 1])
            early = range(halves, num_groups)
            if group == 0:
                waits += state["sends"]
            waits = list(lax.optimization_barrier(tuple(waits)))
            blocks, panels[sup] = waits[:3], waits[3]
            waits = waits[4:]
            if group > 0:
                near[group - 1] = (waits.pop(0), waits.pop(0))
            total = waits.pop(0) if group + 1 in totals else None
            if group == 0:
                state["early"] = collect_lower(waits)
            lowers[group], state["right"], *rest = run_group(
                group, halves, [grad_out, *blocks], panels[sup], right_side, total, state["right"]
            )
            if rest:
                totals[group] = rest[0]
            if group in early:
                sums[group] = lax.psum_scatter(lowers[group], "col", scatter_dimension=0, tiled=True)
            if group == halves:
                state["sends"] = [
                    jnp.concatenate([widen(choose(sums[early_group], turn)) for early_group in early], axis=0)
                    for turn in range(halves)
                ]

        for sup in reversed(range(num_supers)):
            spread_panel(sup)
        send_own(num_groups - 1)
        send_own(num_groups - 2)
        forward(num_groups - 1)
        for group in reversed(range(num_groups)):
            if group > 0:
                forward(group - 1)
            compute(group)

        late = jnp.stack([lowers[group].reshape(mesh_rows, BLOCK_SIZE, -1) for group in range(halves)], axis=1)
        late = lax.psum_scatter(late.reshape(rows_here * 2 * mesh_rows // num_groups, -1), "col", scatter_dimension=0, tiled=True)
        late = by_part(collect_lower([choose(late, turn) for turn in range(halves)]))
        half_size = BLOCK_SIZE // halves
        rest = by_part(state["early"])
        lower_rows = [widen(piece) for piece in late]
        for idx in range(num_groups - halves):
            lower_rows += [piece[idx * half_size:(idx + 1) * half_size] for piece in rest]
        grad_lower = jnp.concatenate(lower_rows, axis=0)
        row_pos = jnp.arange(rows_here)[:, None]
        col_pos = jnp.arange(cols_here)[None, :]
        row_global = (row_pos // BLOCK_SIZE * mesh_rows + lax.axis_index("row")) * BLOCK_SIZE + row_pos % BLOCK_SIZE
        col_global = (col_pos // BLOCK_SIZE * mesh_cols + my_col) * BLOCK_SIZE + col_pos % BLOCK_SIZE
        grad_lower = jnp.where(row_global >= col_global, grad_lower, 0.0).astype(jnp.bfloat16)
        return state["right"], grad_lower

    return jax.shard_map(shards, mesh=mesh, in_specs=(block_spec, block_spec, block_spec), out_specs=(block_spec, block_spec), check_vma=False)
```

```python
import functools

import jax
import jax.numpy as jnp
from jax import lax
from jax.experimental import pallas as pl
from jax.experimental.pallas import tpu as pltpu
from jax.sharding import PartitionSpec as P


BLOCK_SIZE = 256
PIECE = 512
LATE_PIECE = 1024


def seat(rel, mesh_rows):
    return rel % 2 * (mesh_rows // 2) + rel // 2


def group_kernel(group, halves, has_total, *refs):
    refs = list(refs)
    block_refs = [refs.pop(0) for _ in range(4)]
    panel_ref, side_ref = refs.pop(0), refs.pop(0)
    total_ref = refs.pop(0) if has_total else None
    if has_total:
        refs.pop(0)
    lower_ref, right_ref = refs.pop(0), refs.pop(0)
    next_ref = refs.pop(0) if group else None
    turned, rows = refs
    mesh_rows = len(block_refs)
    size = block_refs[0].shape[0]
    turns = lower_ref.shape[1] // (halves * size)

    def place(idx):
        return slice((idx % halves * turns + idx // halves) * size, (idx % halves * turns + idx // halves + 1) * size)

    @pl.when(pl.program_id(0) == 0)
    def _():
        lower_ref[...] = jnp.zeros_like(lower_ref)
        for idx in range(group + 1):
            for rel in range(mesh_rows):
                tile = panel_ref[idx % halves * mesh_rows + seat(rel, mesh_rows), :, idx // halves * size:(idx // halves + 1) * size]
                turned[idx * size:(idx + 1) * size, rel * size:(rel + 1) * size] = tile.T

    for rel in range(mesh_rows):
        rows[rel * size:(rel + 1) * size, :] = block_refs[rel][...]
    for idx in range(group + 1):
        here = slice(idx * size, (idx + 1) * size)
        lower_ref[:, place(idx)] += lax.dot_general(
            rows[...], side_ref[here, :], (((1,), (1,)), ((), ())), preferred_element_type=jnp.float32
        )
        share = jnp.dot(turned[here, :], rows[...], preferred_element_type=jnp.float32)
        if has_total:
            share = total_ref[here, :] + share
        if idx == group:
            right_ref[...] = share.astype(right_ref.dtype)
        else:
            next_ref[here, :] = share


def run_group(group, halves, blocks, panel, side, total, right):
    size = blocks[1].shape[0]
    num_cols = side.shape[1]
    width = (group + 1) * size
    wide = -(-(group + 1) // halves) * halves * size
    depth = panel.shape[1] // halves
    piece = min(PIECE, num_cols)
    has_total = total is not None
    in_specs = [pl.BlockSpec((size, piece), lambda j: (group, j))]
    in_specs += [pl.BlockSpec((size, piece), lambda j: (0, j))] * 3
    in_specs += [
        pl.BlockSpec((panel.shape[0], depth, panel.shape[2]), lambda j: (0, group % halves, 0)),
        pl.BlockSpec((width, piece), lambda j: (0, j)),
    ]
    args = [*blocks, panel, side]
    aliases = {}
    if has_total:
        in_specs += [pl.BlockSpec((width, piece), lambda j: (0, j)), pl.BlockSpec(memory_space=pl.ANY)]
        args += [total, right]
        aliases = {len(args) - 1: 1}
    out_shape = [
        jax.ShapeDtypeStruct((4 * size, wide), jnp.float32),
        jax.ShapeDtypeStruct(side.shape, jnp.bfloat16),
    ]
    out_specs = [
        pl.BlockSpec((4 * size, wide), lambda j: (0, 0)),
        pl.BlockSpec((size, piece), lambda j: (group, j)),
    ]
    if group:
        out_shape.append(jax.ShapeDtypeStruct((group * size, num_cols), jnp.float32))
        out_specs.append(pl.BlockSpec((group * size, piece), lambda j: (0, j)))
    return pl.pallas_call(
        functools.partial(group_kernel, group, halves, has_total),
        grid=(num_cols // piece,),
        in_specs=in_specs,
        out_specs=out_specs,
        out_shape=out_shape,
        scratch_shapes=[pltpu.VMEM((width, 4 * size), jnp.bfloat16), pltpu.VMEM((4 * size, piece), jnp.bfloat16)],
        input_output_aliases=aliases,
        compiler_params=pltpu.CompilerParams(vmem_limit_bytes=56 * 1024 * 1024),
        cost_estimate=pl.CostEstimate(
            flops=4 * 4 * size * width * num_cols, bytes_accessed=num_cols * (12 * size + 10 * width), transcendentals=0
        ),
    )(*args)


def turn_panel(panel_ref, turned, rels, halves, mesh_rows):
    depth, size = panel_ref.shape[1], panel_ref.shape[2]
    for idx in range(halves):
        for turn, rel in enumerate(rels):
            for part in range(depth // size):
                tile = panel_ref[idx * mesh_rows + seat(rel, mesh_rows), part * size:(part + 1) * size, :]
                start = turn * depth + part * size
                turned[idx * size:(idx + 1) * size, start:start + size] = tile.T


def late_near_kernel(halves, own_ref, next_refs, prev_refs, panel_ref, side_ref, total_ref, lower_ref, sum_ref, turned, rows):
    mesh_rows = panel_ref.shape[0] // halves
    depth, size = panel_ref.shape[1], panel_ref.shape[2]
    last = mesh_rows - 1

    @pl.when(pl.program_id(0) == 0)
    def _():
        lower_ref[...] = jnp.zeros_like(lower_ref)
        turn_panel(panel_ref, turned, (0, 1, last), halves, mesh_rows)

    rows[:depth, :] = own_ref[...]
    for part in range(halves):
        rows[depth + part * size:depth + (part + 1) * size, :] = next_refs[part][...]
        rows[2 * depth + part * size:2 * depth + (part + 1) * size, :] = prev_refs[part][...]
    for idx in range(halves):
        here = slice(idx * size, (idx + 1) * size)
        for start, stop, put in ((0, 2 * depth, 0), (2 * depth, 3 * depth, last * depth)):
            lower_ref[put:put + stop - start, here] += lax.dot_general(
                rows[start:stop, :], side_ref[here, :], (((1,), (1,)), ((), ())), preferred_element_type=jnp.float32
            )
        sum_ref[here, :] = total_ref[here, :] + jnp.dot(turned[here, :], rows[...], preferred_element_type=jnp.float32)


def late_far_kernel(halves, far_refs, panel_ref, side_ref, sum_ref, lower_ref, right_ref, turned, rows):
    mesh_rows = panel_ref.shape[0] // halves
    size = panel_ref.shape[2]

    @pl.when(pl.program_id(0) == 0)
    def _():
        lower_ref[...] = jnp.zeros_like(lower_ref)
        turn_panel(panel_ref, turned, (2,), halves, mesh_rows)

    for part in range(halves):
        rows[part * size:(part + 1) * size, :] = far_refs[part][...]
    for idx in range(halves):
        here = slice(idx * size, (idx + 1) * size)
        lower_ref[:, here] += lax.dot_general(
            rows[...], side_ref[here, :], (((1,), (1,)), ((), ())), preferred_element_type=jnp.float32
        )
        share = sum_ref[here, :] + jnp.dot(turned[here, :], rows[...], preferred_element_type=jnp.float32)
        right_ref[here, :] = share.astype(right_ref.dtype)


def run_late_near(halves, own, nexts, prevs, panel, side, total):
    depth, size = panel.shape[1], panel.shape[2]
    mesh_rows = panel.shape[0] // halves
    num_cols = side.shape[1]
    piece = min(LATE_PIECE, num_cols)

    def kernel(own_ref, *refs):
        late_near_kernel(halves, own_ref, refs[:halves], refs[halves:2 * halves], *refs[2 * halves:])

    wide = pl.BlockSpec((depth, piece), lambda j: (0, j))
    return pl.pallas_call(
        kernel,
        name="late_near",
        grid=(num_cols // piece,),
        in_specs=[wide]
        + [pl.BlockSpec((size, piece), lambda j: (0, j))] * (2 * halves)
        + [pl.BlockSpec(panel.shape, lambda j: (0, 0, 0)), wide, wide],
        out_specs=[pl.BlockSpec((mesh_rows * depth, depth), lambda j: (0, 0)), wide],
        out_shape=[
            jax.ShapeDtypeStruct((mesh_rows * depth, depth), jnp.float32),
            jax.ShapeDtypeStruct((depth, num_cols), jnp.float32),
        ],
        scratch_shapes=[pltpu.VMEM((depth, 3 * depth), jnp.bfloat16), pltpu.VMEM((3 * depth, piece), jnp.bfloat16)],
        compiler_params=pltpu.CompilerParams(vmem_limit_bytes=56 * 1024 * 1024),
        cost_estimate=pl.CostEstimate(flops=12 * depth * depth * num_cols, bytes_accessed=16 * depth * num_cols, transcendentals=0),
    )(own, *nexts, *prevs, panel, side, total)


def run_late_far(halves, fars, panel, side, total, lower, right):
    depth, size = panel.shape[1], panel.shape[2]
    num_cols = side.shape[1]
    piece = min(LATE_PIECE, num_cols)

    def kernel(*refs):
        late_far_kernel(halves, refs[:halves], *refs[halves:halves + 3], *refs[halves + 5:])

    wide = pl.BlockSpec((depth, piece), lambda j: (0, j))
    anywhere = pl.BlockSpec(memory_space=pl.ANY)
    return pl.pallas_call(
        kernel,
        name="late_far",
        grid=(num_cols // piece,),
        in_specs=[pl.BlockSpec((size, piece), lambda j: (0, j))] * halves
        + [pl.BlockSpec(panel.shape, lambda j: (0, 0, 0)), wide, wide, anywhere, anywhere],
        out_specs=[pl.BlockSpec((depth, depth), lambda j: (2, 0)), wide],
        out_shape=[jax.ShapeDtypeStruct(lower.shape, jnp.float32), jax.ShapeDtypeStruct(right.shape, jnp.bfloat16)],
        scratch_shapes=[pltpu.VMEM((depth, depth), jnp.bfloat16), pltpu.VMEM((depth, piece), jnp.bfloat16)],
        input_output_aliases={halves + 3: 0, halves + 4: 1},
        compiler_params=pltpu.CompilerParams(vmem_limit_bytes=56 * 1024 * 1024),
        cost_estimate=pl.CostEstimate(flops=4 * depth * depth * num_cols, bytes_accessed=10 * depth * num_cols, transcendentals=0),
    )(*fars, panel, side, total, lower, right)


def solution(mesh):
    mesh_rows = mesh.shape["row"]
    mesh_cols = mesh.shape["col"]
    halves = mesh_cols // mesh_rows
    block_spec = P(("batch", "row"), "col")
    up = [(row, (row + 1) % mesh_rows) for row in range(mesh_rows)]
    down = [(row, (row - 1) % mesh_rows) for row in range(mesh_rows)]

    spread = []
    collect = [[] for _ in range(halves)]
    for row in range(mesh_rows):
        for col in range(mesh_cols):
            home, half = col % mesh_rows, col // mesh_rows
            spread.append((row * mesh_cols + col, home * mesh_cols + half * mesh_rows + seat((row - home) % mesh_rows, mesh_rows)))
            rel, part = col // halves, col % halves
            for turn in range(halves):
                owner = (row + rel) % mesh_rows * mesh_cols + row + mesh_rows * ((part + turn) % halves)
                collect[turn].append((row * mesh_cols + col, owner))

    def shards(lower_tri, right_side, grad_out):
        rows_here, cols_here = lower_tri.shape
        num_groups = rows_here // BLOCK_SIZE
        num_supers = num_groups // halves
        my_col = lax.axis_index("col")
        my_half = my_col // mesh_rows
        my_part = my_col % halves

        own = {num_groups - 1: grad_out[(num_groups - 1) * BLOCK_SIZE:]}
        own[num_groups - 1], grad_later = lax.optimization_barrier((own[num_groups - 1], grad_out))
        for group in range(num_groups - 1):
            own[group] = grad_later[group * BLOCK_SIZE:(group + 1) * BLOCK_SIZE]
        near = {}
        far = {}
        panels = {
            sup: lower_tri[sup * halves * BLOCK_SIZE:(sup + 1) * halves * BLOCK_SIZE, :(sup + 1) * BLOCK_SIZE]
            for sup in range(num_supers)
        }
        totals = {}
        lowers = {}
        sums = {}
        state = {"right": None}

        def send_own(group):
            near[group] = (lax.ppermute(own[group], "row", up), lax.ppermute(own[group], "row", down))

        def spread_panel(sup):
            panel = lax.ppermute(panels[sup], ("row", "col"), spread)
            panels[sup] = lax.all_gather(panel, "col", axis=0)

        def forward(group):
            waits = list(near[group])
            later = group - 2
            if later >= 0:
                waits.append(own[later])
            if group + 2 in totals:
                waits.append(totals[group + 2])
            waits = list(lax.optimization_barrier(tuple(waits)))
            near[group] = (waits.pop(0), waits.pop(0))
            if group % 2:
                far[group] = lax.ppermute(near[group][0], "row", up)
            else:
                far[group] = lax.ppermute(near[group][1], "row", down)
            if later >= 0:
                own[later] = waits.pop(0)
                send_own(later)
            if group + 2 in totals:
                totals[group + 2] = waits.pop(0)

        def choose(values, turn):
            width = values.shape[1] // halves
            chosen = values[:, turn * width:(turn + 1) * width]
            for part in range(1, halves):
                start = (part + turn) % halves * width
                chosen = jnp.where(my_part == part, values[:, start:start + width], chosen)
            return chosen.astype(jnp.bfloat16)

        def collect_lower(sends):
            return [lax.ppermute(send, ("row", "col"), collect[turn]) for turn, send in enumerate(sends)]

        def by_part(turns):
            ordered = []
            for part in range(halves):
                piece = turns[0]
                for turn in range(1, halves):
                    piece = jnp.where((my_half - part) % halves == turn, turns[turn], piece)
                ordered.append(piece)
            return ordered

        def widen(value):
            return jnp.pad(value, ((0, 0), (0, cols_here - value.shape[1])))

        def compute(group):
            sup = group // halves
            waits = [near[group][1], far[group], near[group][0], panels[sup]]
            if group > 0:
                waits += near[group - 1]
            if group + 1 in totals:
                waits.append(totals[group + 1])
            waits = list(lax.optimization_barrier(tuple(waits)))
            blocks, panels[sup] = waits[:3], waits[3]
            waits = waits[4:]
            if group > 0:
                near[group - 1] = (waits.pop(0), waits.pop(0))
            total = waits.pop(0) if group + 1 in totals else None
            lowers[group], state["right"], *rest = run_group(
                group, halves, [grad_out, *blocks], panels[sup], right_side, total, state["right"]
            )
            if rest:
                totals[group] = rest[0]
            sums[group] = lax.psum_scatter(lowers[group], "col", scatter_dimension=0, tiled=True)

        for sup in reversed(range(num_supers)):
            spread_panel(sup)
        send_own(num_groups - 1)
        send_own(num_groups - 2)
        forward(num_groups - 1)
        for group in reversed(range(halves, num_groups)):
            forward(group - 1)
            compute(group)
        for group in reversed(range(halves - 1)):
            forward(group)

        firsts = range(halves)
        waits = lax.optimization_barrier((totals[halves], panels[0], *(block for group in firsts for block in near[group])))
        panel, arrived = waits[1], waits[2:]
        lower, total = run_late_near(halves, grad_out, arrived[1::2], arrived[0::2], panel, right_side, waits[0])
        lower, total, panel, *fars = lax.optimization_barrier((lower, total, panel, *(far[group] for group in firsts)))
        lower, grad_right = run_late_far(halves, fars, panel, right_side, total, lower, state["right"])
        late = lax.psum_scatter(lower, "col", scatter_dimension=0, tiled=True)

        half_size = BLOCK_SIZE // halves
        lower_rows = [widen(piece) for piece in by_part(collect_lower([choose(late, turn) for turn in range(halves)]))]
        for sup in range(1, num_supers):
            groups = range(sup * halves, (sup + 1) * halves)
            turns = collect_lower(
                [jnp.concatenate([choose(sums[group], turn) for group in groups], axis=0) for turn in range(halves)],
            )
            pieces = by_part(turns)
            for idx in range(halves):
                lower_rows += [widen(piece[idx * half_size:(idx + 1) * half_size]) for piece in pieces]
        grad_lower = jnp.concatenate(lower_rows, axis=0)
        row_pos = jnp.arange(rows_here)[:, None]
        col_pos = jnp.arange(cols_here)[None, :]
        row_global = (row_pos // BLOCK_SIZE * mesh_rows + lax.axis_index("row")) * BLOCK_SIZE + row_pos % BLOCK_SIZE
        col_global = (col_pos // BLOCK_SIZE * mesh_cols + my_col) * BLOCK_SIZE + col_pos % BLOCK_SIZE
        grad_lower = jnp.where(row_global >= col_global, grad_lower, 0.0).astype(jnp.bfloat16)
        return grad_right, grad_lower

    return jax.shard_map(shards, mesh=mesh, in_specs=(block_spec, block_spec, block_spec), out_specs=(block_spec, block_spec), check_vma=False)
```

```python
import functools

import jax
import jax.numpy as jnp
from jax import lax
from jax.experimental import pallas as pl
from jax.experimental.pallas import tpu as pltpu
from jax.sharding import PartitionSpec as P


BLOCK_SIZE = 256
PIECE = 512
LATE_PIECE = 1024


def seat(rel, mesh_rows):
    return rel % 2 * (mesh_rows // 2) + rel // 2


def group_kernel(group, halves, has_total, *refs):
    refs = list(refs)
    block_refs = [refs.pop(0) for _ in range(4)]
    panel_ref, side_ref = refs.pop(0), refs.pop(0)
    total_ref = refs.pop(0) if has_total else None
    if has_total:
        refs.pop(0)
    lower_ref, right_ref = refs.pop(0), refs.pop(0)
    next_ref = refs.pop(0) if group else None
    turned, rows = refs
    mesh_rows = len(block_refs)
    size = block_refs[0].shape[0]
    turns = lower_ref.shape[1] // (halves * size)

    def place(idx):
        return slice((idx % halves * turns + idx // halves) * size, (idx % halves * turns + idx // halves + 1) * size)

    @pl.when(pl.program_id(0) == 0)
    def _():
        lower_ref[...] = jnp.zeros_like(lower_ref)
        for idx in range(group + 1):
            for rel in range(mesh_rows):
                tile = panel_ref[idx % halves * mesh_rows + seat(rel, mesh_rows), :, idx // halves * size:(idx // halves + 1) * size]
                turned[idx * size:(idx + 1) * size, rel * size:(rel + 1) * size] = tile.T

    for rel in range(mesh_rows):
        rows[rel * size:(rel + 1) * size, :] = block_refs[rel][...]
    for idx in range(group + 1):
        here = slice(idx * size, (idx + 1) * size)
        lower_ref[:, place(idx)] += lax.dot_general(
            rows[...], side_ref[here, :], (((1,), (1,)), ((), ())), preferred_element_type=jnp.float32
        )
        share = jnp.dot(turned[here, :], rows[...], preferred_element_type=jnp.float32)
        if has_total:
            share = total_ref[here, :] + share
        if idx == group:
            right_ref[...] = share.astype(right_ref.dtype)
        else:
            next_ref[here, :] = share


def run_group(group, halves, blocks, panel, side, total, right):
    size = blocks[1].shape[0]
    num_cols = side.shape[1]
    width = (group + 1) * size
    wide = -(-(group + 1) // halves) * halves * size
    depth = panel.shape[1] // halves
    piece = min(PIECE, num_cols)
    has_total = total is not None
    in_specs = [pl.BlockSpec((size, piece), lambda j: (group, j))]
    in_specs += [pl.BlockSpec((size, piece), lambda j: (0, j))] * 3
    in_specs += [
        pl.BlockSpec((panel.shape[0], depth, panel.shape[2]), lambda j: (0, group % halves, 0)),
        pl.BlockSpec((width, piece), lambda j: (0, j)),
    ]
    args = [*blocks, panel, side]
    aliases = {}
    if has_total:
        in_specs += [pl.BlockSpec((width, piece), lambda j: (0, j)), pl.BlockSpec(memory_space=pl.ANY)]
        args += [total, right]
        aliases = {len(args) - 1: 1}
    out_shape = [
        jax.ShapeDtypeStruct((4 * size, wide), jnp.float32),
        jax.ShapeDtypeStruct(side.shape, jnp.bfloat16),
    ]
    out_specs = [
        pl.BlockSpec((4 * size, wide), lambda j: (0, 0)),
        pl.BlockSpec((size, piece), lambda j: (group, j)),
    ]
    if group:
        out_shape.append(jax.ShapeDtypeStruct((group * size, num_cols), jnp.float32))
        out_specs.append(pl.BlockSpec((group * size, piece), lambda j: (0, j)))
    return pl.pallas_call(
        functools.partial(group_kernel, group, halves, has_total),
        grid=(num_cols // piece,),
        in_specs=in_specs,
        out_specs=out_specs,
        out_shape=out_shape,
        scratch_shapes=[pltpu.VMEM((width, 4 * size), jnp.bfloat16), pltpu.VMEM((4 * size, piece), jnp.bfloat16)],
        input_output_aliases=aliases,
        compiler_params=pltpu.CompilerParams(vmem_limit_bytes=56 * 1024 * 1024),
        cost_estimate=pl.CostEstimate(
            flops=4 * 4 * size * width * num_cols, bytes_accessed=num_cols * (12 * size + 10 * width), transcendentals=0
        ),
    )(*args)


def turn_panel(panel_ref, turned, rels, halves, mesh_rows):
    depth, size = panel_ref.shape[1], panel_ref.shape[2]
    for idx in range(halves):
        for turn, rel in enumerate(rels):
            for part in range(depth // size):
                tile = panel_ref[idx * mesh_rows + seat(rel, mesh_rows), part * size:(part + 1) * size, :]
                start = turn * depth + part * size
                turned[idx * size:(idx + 1) * size, start:start + size] = tile.T


def late_near_kernel(halves, own_ref, next_refs, prev_refs, panel_ref, side_ref, total_ref, lower_ref, sum_ref, turned, rows):
    mesh_rows = panel_ref.shape[0] // halves
    depth, size = panel_ref.shape[1], panel_ref.shape[2]
    last = mesh_rows - 1

    @pl.when(pl.program_id(0) == 0)
    def _():
        lower_ref[...] = jnp.zeros_like(lower_ref)
        turn_panel(panel_ref, turned, (0, 1, last), halves, mesh_rows)

    rows[:depth, :] = own_ref[...]
    for part in range(halves):
        rows[depth + part * size:depth + (part + 1) * size, :] = next_refs[part][...]
        rows[2 * depth + part * size:2 * depth + (part + 1) * size, :] = prev_refs[part][...]
    for idx in range(halves):
        here = slice(idx * size, (idx + 1) * size)
        for start, stop, put in ((0, 2 * depth, 0), (2 * depth, 3 * depth, last * depth)):
            lower_ref[put:put + stop - start, here] += lax.dot_general(
                rows[start:stop, :], side_ref[here, :], (((1,), (1,)), ((), ())), preferred_element_type=jnp.float32
            )
        sum_ref[here, :] = total_ref[here, :] + jnp.dot(turned[here, :], rows[...], preferred_element_type=jnp.float32)


def late_far_kernel(halves, far_refs, panel_ref, side_ref, sum_ref, lower_ref, right_ref, turned, rows):
    mesh_rows = panel_ref.shape[0] // halves
    size = panel_ref.shape[2]

    @pl.when(pl.program_id(0) == 0)
    def _():
        lower_ref[...] = jnp.zeros_like(lower_ref)
        turn_panel(panel_ref, turned, (2,), halves, mesh_rows)

    for part in range(halves):
        rows[part * size:(part + 1) * size, :] = far_refs[part][...]
    for idx in range(halves):
        here = slice(idx * size, (idx + 1) * size)
        lower_ref[:, here] += lax.dot_general(
            rows[...], side_ref[here, :], (((1,), (1,)), ((), ())), preferred_element_type=jnp.float32
        )
        share = sum_ref[here, :] + jnp.dot(turned[here, :], rows[...], preferred_element_type=jnp.float32)
        right_ref[here, :] = share.astype(right_ref.dtype)


def run_late_near(halves, own, nexts, prevs, panel, side, total):
    depth, size = panel.shape[1], panel.shape[2]
    mesh_rows = panel.shape[0] // halves
    num_cols = side.shape[1]
    piece = min(LATE_PIECE, num_cols)

    def kernel(own_ref, *refs):
        late_near_kernel(halves, own_ref, refs[:halves], refs[halves:2 * halves], *refs[2 * halves:])

    wide = pl.BlockSpec((depth, piece), lambda j: (0, j))
    return pl.pallas_call(
        kernel,
        name="late_near",
        grid=(num_cols // piece,),
        in_specs=[wide]
        + [pl.BlockSpec((size, piece), lambda j: (0, j))] * (2 * halves)
        + [pl.BlockSpec(panel.shape, lambda j: (0, 0, 0)), wide, wide],
        out_specs=[pl.BlockSpec((mesh_rows * depth, depth), lambda j: (0, 0)), wide],
        out_shape=[
            jax.ShapeDtypeStruct((mesh_rows * depth, depth), jnp.float32),
            jax.ShapeDtypeStruct((depth, num_cols), jnp.float32),
        ],
        scratch_shapes=[pltpu.VMEM((depth, 3 * depth), jnp.bfloat16), pltpu.VMEM((3 * depth, piece), jnp.bfloat16)],
        compiler_params=pltpu.CompilerParams(vmem_limit_bytes=56 * 1024 * 1024),
        cost_estimate=pl.CostEstimate(flops=12 * depth * depth * num_cols, bytes_accessed=16 * depth * num_cols, transcendentals=0),
    )(own, *nexts, *prevs, panel, side, total)


def run_late_far(halves, fars, panel, side, total, lower, right):
    depth, size = panel.shape[1], panel.shape[2]
    num_cols = side.shape[1]
    piece = min(LATE_PIECE, num_cols)

    def kernel(*refs):
        late_far_kernel(halves, refs[:halves], *refs[halves:halves + 3], *refs[halves + 5:])

    wide = pl.BlockSpec((depth, piece), lambda j: (0, j))
    anywhere = pl.BlockSpec(memory_space=pl.ANY)
    return pl.pallas_call(
        kernel,
        name="late_far",
        grid=(num_cols // piece,),
        in_specs=[pl.BlockSpec((size, piece), lambda j: (0, j))] * halves
        + [pl.BlockSpec(panel.shape, lambda j: (0, 0, 0)), wide, wide, anywhere, anywhere],
        out_specs=[pl.BlockSpec((depth, depth), lambda j: (2, 0)), wide],
        out_shape=[jax.ShapeDtypeStruct(lower.shape, jnp.float32), jax.ShapeDtypeStruct(right.shape, jnp.bfloat16)],
        scratch_shapes=[pltpu.VMEM((depth, depth), jnp.bfloat16), pltpu.VMEM((depth, piece), jnp.bfloat16)],
        input_output_aliases={halves + 3: 0, halves + 4: 1},
        compiler_params=pltpu.CompilerParams(vmem_limit_bytes=56 * 1024 * 1024),
        cost_estimate=pl.CostEstimate(flops=4 * depth * depth * num_cols, bytes_accessed=10 * depth * num_cols, transcendentals=0),
    )(*fars, panel, side, total, lower, right)


def solution(mesh):
    mesh_rows = mesh.shape["row"]
    mesh_cols = mesh.shape["col"]
    halves = mesh_cols // mesh_rows
    block_spec = P(("batch", "row"), "col")
    up = [(row, (row + 1) % mesh_rows) for row in range(mesh_rows)]
    down = [(row, (row - 1) % mesh_rows) for row in range(mesh_rows)]

    spread = []
    collect = [[] for _ in range(halves)]
    for row in range(mesh_rows):
        for col in range(mesh_cols):
            home, half = col % mesh_rows, col // mesh_rows
            spread.append((row * mesh_cols + col, home * mesh_cols + half * mesh_rows + seat((row - home) % mesh_rows, mesh_rows)))
            rel, part = col // halves, col % halves
            for turn in range(halves):
                owner = (row + rel) % mesh_rows * mesh_cols + row + mesh_rows * ((part + turn) % halves)
                collect[turn].append((row * mesh_cols + col, owner))

    def shards(lower_tri, right_side, grad_out):
        rows_here, cols_here = lower_tri.shape
        num_groups = rows_here // BLOCK_SIZE
        num_supers = num_groups // halves
        my_col = lax.axis_index("col")
        my_half = my_col // mesh_rows
        my_part = my_col % halves

        own = {num_groups - 1: grad_out[(num_groups - 1) * BLOCK_SIZE:]}
        own[num_groups - 1], grad_later = lax.optimization_barrier((own[num_groups - 1], grad_out))
        for group in range(num_groups - 1):
            own[group] = grad_later[group * BLOCK_SIZE:(group + 1) * BLOCK_SIZE]
        near = {}
        far = {}
        panels = {
            sup: lower_tri[sup * halves * BLOCK_SIZE:(sup + 1) * halves * BLOCK_SIZE, :(sup + 1) * BLOCK_SIZE]
            for sup in range(num_supers)
        }
        totals = {}
        lowers = {}
        sums = {}
        state = {"right": None}

        def send_own(group):
            near[group] = (lax.ppermute(own[group], "row", up), lax.ppermute(own[group], "row", down))

        def spread_panel(sup):
            panel = lax.ppermute(panels[sup], ("row", "col"), spread)
            panels[sup] = lax.all_gather(panel, "col", axis=0)

        def forward(group):
            waits = list(near[group])
            later = group - 2
            if later >= 0:
                waits.append(own[later])
            if group + 2 in totals:
                waits.append(totals[group + 2])
            waits = list(lax.optimization_barrier(tuple(waits)))
            near[group] = (waits.pop(0), waits.pop(0))
            if group % 2:
                far[group] = lax.ppermute(near[group][0], "row", up)
            else:
                far[group] = lax.ppermute(near[group][1], "row", down)
            if later >= 0:
                own[later] = waits.pop(0)
                send_own(later)
            if group + 2 in totals:
                totals[group + 2] = waits.pop(0)

        def choose(values, turn):
            width = values.shape[1] // halves
            chosen = values[:, turn * width:(turn + 1) * width]
            for part in range(1, halves):
                start = (part + turn) % halves * width
                chosen = jnp.where(my_part == part, values[:, start:start + width], chosen)
            return chosen.astype(jnp.bfloat16)

        def collect_lower(sends):
            return [lax.ppermute(send, ("row", "col"), collect[turn]) for turn, send in enumerate(sends)]

        def by_part(turns):
            ordered = []
            for part in range(halves):
                piece = turns[0]
                for turn in range(1, halves):
                    piece = jnp.where((my_half - part) % halves == turn, turns[turn], piece)
                ordered.append(piece)
            return ordered

        def widen(value):
            return jnp.pad(value, ((0, 0), (0, cols_here - value.shape[1])))

        def compute(group):
            sup = group // halves
            waits = [near[group][1], far[group], near[group][0], panels[sup]]
            if group > 0:
                waits += near[group - 1]
            if group + 1 in totals:
                waits.append(totals[group + 1])
            waits = list(lax.optimization_barrier(tuple(waits)))
            blocks, panels[sup] = waits[:3], waits[3]
            waits = waits[4:]
            if group > 0:
                near[group - 1] = (waits.pop(0), waits.pop(0))
            total = waits.pop(0) if group + 1 in totals else None
            lowers[group], state["right"], *rest = run_group(
                group, halves, [grad_out, *blocks], panels[sup], right_side, total, state["right"]
            )
            if rest:
                totals[group] = rest[0]
            sums[group] = lax.psum_scatter(lowers[group], "col", scatter_dimension=0, tiled=True)

        for sup in reversed(range(num_supers)):
            spread_panel(sup)
        send_own(num_groups - 1)
        send_own(num_groups - 2)
        forward(num_groups - 1)
        for group in reversed(range(halves, num_groups)):
            forward(group - 1)
            compute(group)
        for group in reversed(range(halves - 1)):
            forward(group)

        firsts = range(halves)
        waits = lax.optimization_barrier((totals[halves], panels[0], *(block for group in firsts for block in near[group])))
        panel, arrived = waits[1], waits[2:]
        lower, total = run_late_near(halves, grad_out, arrived[1::2], arrived[0::2], panel, right_side, waits[0])
        lower, total, panel, *fars = lax.optimization_barrier((lower, total, panel, *(far[group] for group in firsts)))
        lower, grad_right = run_late_far(halves, fars, panel, right_side, total, lower, state["right"])
        late = lax.psum_scatter(lower, "col", scatter_dimension=0, tiled=True)

        turns = []
        for sup in range(1, num_supers):
            groups = range(sup * halves, (sup + 1) * halves)
            turns += collect_lower(
                [jnp.concatenate([choose(sums[group], turn) for group in groups], axis=0) for turn in range(halves)],
            )
        late, *turns = lax.optimization_barrier((late, *turns))
        half_size = BLOCK_SIZE // halves
        lower_rows = [widen(piece) for piece in by_part(collect_lower([choose(late, turn) for turn in range(halves)]))]
        for sup in range(1, num_supers):
            pieces = by_part(turns[(sup - 1) * halves:sup * halves])
            for idx in range(halves):
                lower_rows += [widen(piece[idx * half_size:(idx + 1) * half_size]) for piece in pieces]
        grad_lower = jnp.concatenate(lower_rows, axis=0)
        row_pos = jnp.arange(rows_here)[:, None]
        col_pos = jnp.arange(cols_here)[None, :]
        row_global = (row_pos // BLOCK_SIZE * mesh_rows + lax.axis_index("row")) * BLOCK_SIZE + row_pos % BLOCK_SIZE
        col_global = (col_pos // BLOCK_SIZE * mesh_cols + my_col) * BLOCK_SIZE + col_pos % BLOCK_SIZE
        grad_lower = jnp.where(row_global >= col_global, grad_lower, 0.0).astype(jnp.bfloat16)
        return grad_right, grad_lower

    return jax.shard_map(shards, mesh=mesh, in_specs=(block_spec, block_spec, block_spec), out_specs=(block_spec, block_spec), check_vma=False)
```
